512 devices in a mesh: member: 2 (over y), gy: 16 (over z), gx: 8 (over x), lev: 2 (over core).
Axes of the slice: x: 8, y: 2, z: 16, core: 2. Of those that a mesh axis runs over, the one named last changes fastest.
The devices are a block of a 8x8x16 slice.
Arguments:
- level_field: bfloat16 [32, 1536, 1536], P(('member', 'lev'), 'gy', 'gx'), parts along dimension 0, may hold values from -6 to 6
Outputs:
- spectra: float32 [1536, 32, 1536], P(('gy', 'gx'), ('member', 'lev')), parts along dimension 1
- spectra_zone: float32 [1536, 32, 11], P(('gy', 'gx'), ('member', 'lev')), parts along dimension 1
The draws below stay inside these ranges and needn't reach their ends.
There are 2 independent parts, one for each index of `member`. The reference program is written for one: setup_inputs(seed, part) draws one part's arguments, and reference() takes and returns one part's arrays. A program takes and returns all parts, laid end to end along the dimension named above; each array names one. Nothing has to cross between parts.
All inputs are finite; a program needn't handle non-finite values.
Results may differ from the reference program's by a relative error of at most 0.0042.
Values may be sent and summed in bfloat16 or wider, within the bound.
No kernel may reach another device: no remote copies, remote signals or barrier semaphores. Data moves between devices by JAX's collectives and lax.ppermute only.
A program may use at most 64 MiB of HBM per device.

```python
import math
import jax
import jax.numpy as jnp
from jax import lax

NX = 1536
NY = 1536
EXT_ZONE = 11
WAVES = 768
LEVELS = 16


def shard_levels(own_key, shape, cuts, low, largest):
    gain, own = 1.0, jax.random.fold_in(own_key, 6)
    for axis_at, parts in cuts:
        draws = jnp.exp(jax.random.uniform(jax.random.fold_in(own, axis_at), (parts,), jnp.float32, low / len(cuts), largest / len(cuts)))
        gain = gain * jnp.repeat(draws, shape[axis_at] // parts).reshape([-1 if axis == axis_at else 1 for axis in range(len(shape))])
    return gain


def centred(stream_key, dims, deviation, most, split=(), kind=jnp.bfloat16):
    drawn = deviation * jax.random.normal(stream_key, dims, jnp.float32)
    if split:
        drawn = drawn * shard_levels(stream_key, dims, split, -0.22, 0.18)
    return jnp.clip(drawn, -most, most).astype(kind)


def setup_inputs(seed: int = 0, part: int = 0) -> dict:
    keys = jax.random.split(jax.random.key(seed), 2)
    part_splits = jax.random.split(jax.random.fold_in(keys[1], part), 2)
    return {
        "level_field": centred(part_splits[0], (LEVELS, NY, NX), 1.0, 6.0, ((0, 2), (1, 16), (2, 8))),
    }


def blend_zone(second_last, last_value, first_value, second_value, zone_count):
    steps = (jnp.arange(zone_count, dtype=jnp.int32) + 1).astype(jnp.float32) / (zone_count + 1.0)
    weight_a = 2.0 * steps ** 3 - 3.0 * steps ** 2 + 1.0
    weight_b = steps ** 3 - 2.0 * steps ** 2 + steps
    weight_c = -2.0 * steps ** 3 + 3.0 * steps ** 2
    weight_d = steps ** 3 - steps ** 2
    tangent_scale = zone_count + 1.0
    slope_start = tangent_scale * (last_value - second_last)
    slope_end = tangent_scale * (second_value - first_value)
    return last_value[..., None] * weight_a + slope_start[..., None] * weight_b + first_value[..., None] * weight_c + slope_end[..., None] * weight_d

def make_table(wave_count, length):
    coeff = jnp.arange(2 * wave_count, dtype=jnp.int32)[:, None]
    column = jnp.arange(length, dtype=jnp.int32)[None, :]
    is_cosine = coeff < wave_count
    number = jnp.where(is_cosine, coeff, coeff - wave_count + 1)
    phase = (number * column % length).astype(jnp.float32) * (2.0 * math.pi / length)
    values = jnp.where(is_cosine, jnp.cos(phase), -jnp.sin(phase)) / math.sqrt(length)
    return values.astype(jnp.bfloat16)

def reference(level_field):
    widened = level_field.astype(jnp.float32)
    zone_x = blend_zone(widened[..., NX - 2], widened[..., NX - 1], widened[..., 0], widened[..., 1], EXT_ZONE).astype(jnp.bfloat16)
    extended = jnp.concatenate([level_field, zone_x], axis=2)
    wave_table = make_table(WAVES, NX + EXT_ZONE)

    def one_level(level_rows):
        return lax.dot_general(wave_table, level_rows, (((1,), (1,)), ((), ())), preferred_element_type=jnp.float32)
    stacked = lax.map(one_level, extended)
    spectra = jnp.transpose(stacked, (1, 0, 2))
    spectra_zone = blend_zone(spectra[..., NY - 2], spectra[..., NY - 1], spectra[..., 0], spectra[..., 1], EXT_ZONE)
    return (spectra, spectra_zone)
```

```python
import functools
import math

import jax
import jax.numpy as jnp
from jax import lax
from jax.experimental import pallas as pl
from jax.experimental.pallas import tpu as pltpu
from jax.sharding import Mesh, PartitionSpec as P

EXT_ZONE = 11
LANES = 128
HALF = LANES // 2
ROWS = 8
UNROLL = 4
INTERPRET = False


def blend(second_last, last_value, first_value, second_value, steps):
    weight_a = 2.0 * steps * steps * steps - 3.0 * steps * steps + 1.0
    weight_b = steps * steps * steps - 2.0 * steps * steps + steps
    weight_c = -2.0 * steps * steps * steps + 3.0 * steps * steps
    weight_d = steps * steps * steps - steps * steps
    scale = EXT_ZONE + 1.0
    slope_start = scale * (last_value - second_last)
    slope_end = scale * (second_value - first_value)
    return last_value * weight_a + slope_start * weight_b + first_value * weight_c + slope_end * weight_d


def sin_cos(turns, length):
    turns = turns - length * jnp.round(turns * (1.0 / length))
    half = turns * (math.pi / length)
    sq = half * half
    s = sq * (-1.0 / 39916800.0) + 1.0 / 362880.0
    s = s * sq - 1.0 / 5040.0
    s = s * sq + 1.0 / 120.0
    s = s * sq - 1.0 / 6.0
    s = (s * sq + 1.0) * half
    c = sq * (1.0 / 479001600.0) - 1.0 / 3628800.0
    c = c * sq + 1.0 / 40320.0
    c = c * sq - 1.0 / 720.0
    c = c * sq + 1.0 / 24.0
    c = c * sq - 0.5
    c = c * sq + 1.0
    return 2.0 * s * c, 1.0 - 2.0 * s * s


def lane_iota(shape):
    return lax.broadcasted_iota(jnp.int32, shape, 1)


def row_iota(shape):
    return lax.broadcasted_iota(jnp.int32, shape, 0)


def turned(p, q, angle):
    s, c = angle
    return p * c - q * s, q * c + p * s


def twice(angle):
    s, c = angle
    return 2.0 * s * c, 1.0 - 2.0 * s * s


def pack_kernel(field_hbm, out_hbm, field_ref, packed_ref, arrived, sent):
    levels, lats, _ = field_ref.shape
    pairs = levels // 2
    copies = out_hbm.shape[0] // pairs

    def fetch(level):
        return pltpu.make_async_copy(field_hbm.at[level], field_ref.at[level], arrived.at[level])

    def send(pair, copy):
        at = copy * pairs + pair
        return pltpu.make_async_copy(packed_ref.at[pair], out_hbm.at[at], sent.at[at])

    for pair in range(pairs):
        fetch(pair).start()
        fetch(pair + pairs).start()
    for pair in range(pairs):
        fetch(pair).wait()
        fetch(pair + pairs).wait()
        near, far = field_ref[pair], field_ref[pair + pairs]
        rest = [v[:, LANES:].astype(jnp.float32) for v in (near, far)]
        packed_ref[pair, :lats, :] = near[:, :LANES]
        packed_ref[pair, lats : 2 * lats, :] = far[:, :LANES]
        packed_ref[pair, 2 * lats :, :] = jnp.concatenate(rest, axis=1).astype(packed_ref.dtype)
        for copy in range(copies):
            send(pair, copy).start()
    for pair in range(pairs):
        for copy in range(copies):
            send(pair, copy).wait()


def table_kernel(half_ref, table_ref, *, bands, blocks, quarter, share, cols):
    length = blocks * cols + EXT_ZONE
    span = share * blocks
    here = share * quarter
    waves = span * bands // 2
    tile = 2 * ROWS
    row = row_iota((tile, LANES))
    lane = lane_iota((tile, LANES))
    lane_f = lane.astype(jnp.float32)
    start = half_ref[0] * here
    scale = 1.0 / math.sqrt(length)
    left = lane < HALF
    per_band = here // tile

    def rows(n, _):
        coeff = start + span * (n // per_band) + tile * (n % per_band) + row
        is_cosine = coeff < waves
        number = jnp.where(is_cosine, coeff, coeff - (waves - 1)).astype(jnp.float32)
        s0, c0 = sin_cos(number * lane_f, float(length))
        by_half = jnp.broadcast_to(s0[:, HALF : HALF + 1], s0.shape), jnp.broadcast_to(c0[:, HALF : HALF + 1], c0.shape)
        s0, c0 = s0 * scale, c0 * scale
        p = jnp.where(is_cosine, c0, -s0)
        q = jnp.where(is_cosine, s0, c0)
        by_lanes = twice(by_half)
        by_block = turned(by_lanes[1], by_lanes[0], by_half)[::-1]
        by_pair = twice(by_block)
        near, far = turned(p, q, by_lanes), turned(p, q, twice(by_lanes))
        p2, q2 = jnp.where(left, near[0], far[0]), jnp.where(left, near[1], far[1])
        firsts = [p, turned(p, q, by_block)[0]]
        step = 2.0 * by_block[1]
        for _ in range(blocks - 1):
            firsts.append(step * firsts[-1] - firsts[-2])
        rests = [p2, turned(p2, q2, by_pair)[0]]
        step = 2.0 * by_pair[1]
        for _ in range(blocks // 2 - 2):
            rests.append(step * rests[-1] - rests[-2])
        at = pl.ds(pl.multiple_of(n * tile, tile), tile)
        for k, value in enumerate(firsts + rests):
            table_ref[at, k * LANES : (k + 1) * LANES] = value.astype(table_ref.dtype)
        return 0

    lax.fori_loop(0, table_ref.shape[0] // tile, rows, 0, unroll=UNROLL)


def transform_kernel(core_ref, table_ref, out_ref, rows_ref, values_ref, wide_ref, *, lats, cols, share):
    blocks = core_ref.shape[0]
    over = cols - LANES
    lane = lane_iota((lats, LANES))
    left = lane < HALF
    for level in range(2):
        lo = level * LANES
        rows_ref[lo + lats : lo + LANES, :] = jnp.zeros((LANES - lats, rows_ref.shape[1]), rows_ref.dtype)
        for b in range(blocks):
            rows_ref[lo : lo + lats, b * LANES : (b + 1) * LANES] = core_ref[b, level * lats : (level + 1) * lats, :]
    first_rest = blocks + 1
    for pair in range(blocks // 2):
        even = core_ref[2 * pair, 2 * lats :, :].astype(jnp.float32)
        odd = core_ref[2 * pair + 1, 2 * lats :, :].astype(jnp.float32)
        merged = (jnp.where(left, even, pltpu.roll(odd, HALF, 1)), jnp.where(left, pltpu.roll(even, HALF, 1), odd))
        at = (first_rest + pair) * LANES
        for level in range(2):
            rows_ref[level * LANES : level * LANES + lats, at : at + LANES] = merged[level].astype(rows_ref.dtype)
    steps = (lane + 1).astype(jnp.float32) / (EXT_ZONE + 1.0)
    last = core_ref[blocks - 1, 2 * lats :, :].astype(jnp.float32)
    for level in range(2):
        head = core_ref[0, level * lats : (level + 1) * lats, :].astype(jnp.float32)
        end = level * HALF + over
        zone = blend(last[:, end - 2 : end - 1], last[:, end - 1 : end], head[:, 0:1], head[:, 1:2], steps)
        zone = jnp.where(lane < EXT_ZONE, zone, 0.0)
        rows_ref[level * LANES : level * LANES + lats, blocks * LANES : first_rest * LANES] = zone.astype(rows_ref.dtype)

    count = values_ref.shape[0]
    size = wide_ref.shape[0]
    piece = LANES - lats
    six = share // 2

    def one(chunk, _):
        at = pl.ds(pl.multiple_of(chunk * count, count), count)
        values_ref[...] = lax.dot_general(
            table_ref[at, :], rows_ref[...], (((1,), (1,)), ((), ())), preferred_element_type=jnp.float32
        )
        for m in range(count // share):
            lo, to = m * share, m * 3 * six
            wide_ref[to : to + share, :] = values_ref[lo : lo + share, :LANES]
            wide_ref[to + share : to + 3 * six, :] = values_ref[lo : lo + six, LANES:]
            rest = values_ref[lo + six : lo + share, LANES:]
            for j in range(3):
                moved = pltpu.roll(rest, lats - piece * j, 1)
                wide_ref[to + six * j : to + six * (j + 1), lats:] = moved[:, lats:]
        out_ref[pl.ds(pl.multiple_of(chunk * size, size), size), :] = wide_ref[...].astype(out_ref.dtype)
        return 0

    lax.fori_loop(0, table_ref.shape[0] // count, one, 0)


def unpack_kernel(in_ref, out_ref, zone_ref, wide_ref, *, lats):
    share, levels, total = out_ref.shape
    pairs = levels // 2
    six = share // 2
    stride = 3 * six
    bands = in_ref.shape[0] // (pairs * stride)
    piece = LANES - lats
    lane = lane_iota((levels, LANES))
    upper = row_iota((levels, LANES)) < pairs
    wide_ref[...] = in_ref[...].astype(jnp.float32)

    def rolled(value, shift):
        return value if shift % LANES == 0 else pltpu.roll(value, shift % LANES, 1)

    def picked(g, at):
        return wide_ref[pl.ds(g * pairs * stride + at, levels, stride=stride), :]

    ends = [jnp.zeros((levels, LANES), jnp.float32) for _ in range(4)]
    for c in range(share):
        first = last = held = None
        fill = 0
        for g in range(0, bands, 2):
            near = picked(g, c)
            if c < six:
                far = picked(g, share + c)
            else:
                parts = [rolled(picked(g, six * j + c - six), piece * j - lats) for j in range(3)]
                far = jnp.where(lane < piece, parts[0], jnp.where(lane < 2 * piece, parts[1], parts[2]))
            both = (
                jnp.where(upper, near, pltpu.roll(far, pairs, 0)),
                jnp.where(upper, pltpu.roll(near, pairs, 0), far),
            )
            for e, value in enumerate(both):
                moved = rolled(value, (g + e) * lats)
                tile = (g + e) * lats // LANES
                current = moved if fill == 0 else jnp.where(lane < fill, held, moved)
                fill += lats
                if fill >= LANES:
                    out_ref[c, :, tile * LANES : (tile + 1) * LANES] = current
                    first = current if tile == 0 else first
                    last = current
                    fill -= LANES
                    held = moved
                else:
                    held = current
        for e, (source, at) in enumerate(((last, LANES - 2), (last, LANES - 1), (first, 0), (first, 1))):
            ends[e] = jnp.where(lane == c, rolled(source, c - at), ends[e])
    for j in range(EXT_ZONE):
        step = jnp.full((levels, LANES), float(j + 1), jnp.float32) / (EXT_ZONE + 1.0)
        zone_ref[j] = blend(*ends, step)[:, :share]


def call(kernel, out_shape, scratch=(), limit=16 << 20, **static):
    return pl.pallas_call(
        functools.partial(kernel, **static),
        out_shape=out_shape,
        scratch_shapes=list(scratch),
        compiler_params=pltpu.CompilerParams(vmem_limit_bytes=limit),
        interpret=INTERPRET,
        name=kernel.__name__,
    )


def shards(level_field):
    halves, quarter = lax.axis_size("gx_half"), lax.axis_size("gx_quarter")
    blocks = halves * quarter
    bands = lax.axis_size("gy")
    levels, lats, cols = level_field.shape
    share = cols // bands
    six = share // 2
    bf16, f32 = jnp.bfloat16, jnp.float32
    assert share * bands == cols and levels == 2 * quarter and halves == 2 and cols == LANES + HALF
    assert share == 2 * six and lats == 3 * (LANES - lats) and bands % 2 == 0 and levels == ROWS

    half = lax.axis_index("gx_half").astype(jnp.int32).reshape(1)
    packed = pl.pallas_call(
        pack_kernel,
        out_shape=jax.ShapeDtypeStruct((blocks, 3 * lats, LANES), bf16),
        in_specs=[pl.BlockSpec(memory_space=pl.ANY)],
        out_specs=pl.BlockSpec(memory_space=pl.ANY),
        scratch_shapes=[
            pltpu.VMEM(level_field.shape, bf16),
            pltpu.VMEM((levels // 2, 3 * lats, LANES), bf16),
            pltpu.SemaphoreType.DMA((levels,)),
            pltpu.SemaphoreType.DMA((blocks,)),
        ],
        compiler_params=pltpu.CompilerParams(vmem_limit_bytes=60 * 1024 * 1024),
        interpret=INTERPRET,
        name="pack_kernel",
    )(level_field)
    core = lax.all_to_all(packed, ("gx_half", "gx_quarter"), split_axis=0, concat_axis=0, tiled=True)
    width = (blocks + 1 + blocks // 2) * LANES
    table = pl.pallas_call(
        functools.partial(table_kernel, bands=bands, blocks=blocks, quarter=quarter, share=share, cols=cols),
        out_shape=jax.ShapeDtypeStruct((share * quarter * bands, width), bf16),
        in_specs=[pl.BlockSpec(memory_space=pltpu.SMEM)],
        compiler_params=pltpu.CompilerParams(vmem_limit_bytes=8 << 20),
        interpret=INTERPRET,
        name="table_kernel",
    )(half)
    dests = bands * quarter
    chunk = dests // 4
    sent = call(
        transform_kernel,
        jax.ShapeDtypeStruct((dests * 3 * six, LANES), bf16),
        scratch=[
            pltpu.VMEM((2 * LANES, width), bf16),
            pltpu.VMEM((chunk * share, 2 * LANES), f32),
            pltpu.VMEM((chunk * 3 * six, LANES), f32),
        ],
        lats=lats,
        cols=cols,
        share=share,
    )(core, table)
    sent = sent.reshape(dests, 3 * six // 2, 2, LANES)
    sent = lax.all_to_all(sent, ("gy", "gx_quarter"), split_axis=0, concat_axis=0, tiled=True)
    sent = sent.reshape(dests * 3 * six, LANES)
    spectra, zone = call(
        unpack_kernel,
        (
            jax.ShapeDtypeStruct((share, levels, lats * bands), f32),
            jax.ShapeDtypeStruct((EXT_ZONE, levels, share), f32),
        ),
        scratch=[pltpu.VMEM((dests * 3 * six, LANES), f32)],
        lats=lats,
    )(sent)
    return spectra, jnp.transpose(zone, (2, 1, 0))


def solution(mesh):
    members, bands, blocks, cores = (mesh.shape[name] for name in ("member", "gy", "gx", "lev"))
    split = Mesh(
        mesh.devices.reshape(members, bands, 2, blocks // 2, cores), ("member", "gy", "gx_half", "gx_quarter", "lev")
    )
    columns = ("gx_half", "gx_quarter")
    coefficients = P(("gy", *columns), ("member", "lev"), None)
    return jax.shard_map(
        shards,
        mesh=split,
        in_specs=(P(("member", "lev"), "gy", columns),),
        out_specs=(coefficients, coefficients),
        check_vma=False,
    )
```

```python
import functools
import math

import jax
import jax.numpy as jnp
from jax import lax
from jax.experimental import pallas as pl
from jax.experimental.pallas import tpu as pltpu
from jax.sharding import PartitionSpec as P

EXT_ZONE = 11
LANES = 128
ROWS = 8
TILE = 2 * ROWS
UNROLL = 4
PACK_UNROLL = 16
INTERPRET = False


def blend(second_last, last_value, first_value, second_value, steps):
    weight_a = 2.0 * steps * steps * steps - 3.0 * steps * steps + 1.0
    weight_b = steps * steps * steps - 2.0 * steps * steps + steps
    weight_c = -2.0 * steps * steps * steps + 3.0 * steps * steps
    weight_d = steps * steps * steps - steps * steps
    scale = EXT_ZONE + 1.0
    slope_start = scale * (last_value - second_last)
    slope_end = scale * (second_value - first_value)
    return last_value * weight_a + slope_start * weight_b + first_value * weight_c + slope_end * weight_d


def sin_cos(turns, length):
    turns = turns - length * jnp.round(turns * (1.0 / length))
    half = turns * (math.pi / length)
    sq = half * half
    s = sq * (-1.0 / 39916800.0) + 1.0 / 362880.0
    s = s * sq - 1.0 / 5040.0
    s = s * sq + 1.0 / 120.0
    s = s * sq - 1.0 / 6.0
    s = (s * sq + 1.0) * half
    c = sq * (1.0 / 479001600.0) - 1.0 / 3628800.0
    c = c * sq + 1.0 / 40320.0
    c = c * sq - 1.0 / 720.0
    c = c * sq + 1.0 / 24.0
    c = c * sq - 0.5
    c = c * sq + 1.0
    return 2.0 * s * c, 1.0 - 2.0 * s * s


def lane_iota(shape):
    return lax.broadcasted_iota(jnp.int32, shape, 1)


def row_iota(shape):
    return lax.broadcasted_iota(jnp.int32, shape, 0)


def turned(at, by):
    c, s = at
    cb, sb = by
    return c * cb - s * sb, s * cb + c * sb


def twice(angle):
    c, s = angle
    return 1.0 - 2.0 * s * s, 2.0 * s * c


def table_kernel(table_ref, *, blocks, cols, chunk):
    length = blocks * cols + EXT_ZONE
    waves = blocks * cols // 2
    lane = lane_iota((TILE, LANES)).astype(jnp.float32)
    row = row_iota((TILE, LANES))
    scale = 1.0 / math.sqrt(length)

    def pairs(number):
        s, c = sin_cos(number * lane, float(length))
        mid = LANES // 2
        by_mid = jnp.broadcast_to(c[:, mid : mid + 1], c.shape), jnp.broadcast_to(s[:, mid : mid + 1], s.shape)
        by_lanes = twice(by_mid)
        by_block = turned(by_lanes, by_mid)
        near = (c * scale, s * scale)
        far = turned(near, by_lanes)
        side = turned(far, by_lanes)
        left = lane < float(mid)
        halves = blocks // 2
        yield halves * LANES, tuple(jnp.where(left, f, e) for f, e in zip(far, side))
        for b in range(halves):
            yield b * LANES, near
            if b >= 2:
                yield (halves + b - 1) * LANES, far
            near, far = turned(near, by_block), turned(far, by_block)

    per = chunk // TILE

    def rows(n, _):
        first = n // per * (2 * chunk) + n % per * TILE
        for lo, (c, s) in pairs((n * TILE + row).astype(jnp.float32)):
            for part, value in enumerate((c, -s)):
                at = pl.ds(pl.multiple_of(first + part * chunk, TILE), TILE)
                table_ref[at, lo : lo + LANES] = value.astype(table_ref.dtype)
        return 0

    lax.fori_loop(0, waves // TILE, rows, 0, unroll=UNROLL)
    for lo, (c, s) in pairs((waves + row % ROWS).astype(jnp.float32)):
        table_ref[2 * waves :, lo : lo + LANES] = jnp.where(row < ROWS, c, -s).astype(table_ref.dtype)


def transform_kernel(core_ref, table_ref, out_ref, rows_ref, turn_ref, values_ref, wide_ref, *, chunk, share, sent):
    blocks, lats, cols = core_ref.shape
    halves = blocks // 2
    length = blocks * cols + EXT_ZONE
    waves = blocks * cols // 2
    over = cols - LANES
    lane = lane_iota((lats, LANES))
    head = core_ref[0, :, :LANES].astype(jnp.float32)
    steps = (lane - over + 1).astype(jnp.float32) / (EXT_ZONE + 1.0)
    for part in range(2):
        lo = part * LANES
        rows_ref[lo + lats : lo + LANES, :] = jnp.zeros((LANES - lats, rows_ref.shape[1]), rows_ref.dtype)

        def place(tile, value):
            rows_ref[lo : lo + lats, tile * LANES : (tile + 1) * LANES] = value.astype(rows_ref.dtype)

        def others(b):
            value = core_ref[part * halves + b, :, LANES:].astype(jnp.float32)
            return jnp.concatenate([value, jnp.zeros((lats, LANES - over), jnp.float32)], axis=1)

        for b in range(halves):
            place(b, core_ref[part * halves + b, :, :LANES])
        place(halves, others(0) + pltpu.roll(others(1), over, 1))
        for b in range(2, halves):
            value = others(b)
            if part == 1 and b == halves - 1:
                zone = blend(value[:, over - 2 : over - 1], value[:, over - 1 : over], head[:, 0:1], head[:, 1:2], steps)
                value = jnp.where((lane >= over) & (lane < over + EXT_ZONE), zone, value)
            place(halves + b - 1, value)

    shift = float(halves * cols)
    s, c = sin_cos(row_iota((chunk, LANES)).astype(jnp.float32) * shift, float(length))
    turn_ref[0], turn_ref[1] = c, s
    step = 2.0 * math.pi * (chunk * halves * cols % length) / length
    step = math.cos(step), math.sin(step)

    def both(at, count, by):
        values = lax.dot_general(
            table_ref[at, :], rows_ref[...], (((1,), (1,)), ((), ())), preferred_element_type=jnp.float32
        )
        cb, sb = by
        c, s = values[: count // 2], values[count // 2 :]
        c_far, s_far = c[:, LANES:], s[:, LANES:]
        return c[:, :LANES] + (cb * c_far + sb * s_far), s[:, :LANES] + (cb * s_far - sb * c_far)

    def one(n, _):
        by = turn_ref[0], turn_ref[1]
        c, s = both(pl.ds(pl.multiple_of(n * (2 * chunk), 2 * chunk), 2 * chunk), 2 * chunk, by)
        values_ref[pl.ds(waves - 1 + n * chunk, chunk), :] = s
        values_ref[pl.ds(pl.multiple_of(n * chunk, chunk), chunk), :] = c
        turn_ref[0], turn_ref[1] = turned(by, step)
        return 0

    lax.fori_loop(0, waves // chunk, one, 0, unroll=2)
    by = turn_ref[0, :ROWS], turn_ref[1, :ROWS]
    values_ref[2 * waves - 1 : 2 * waves - 1 + ROWS, :] = both(slice(2 * waves, 2 * waves + TILE), TILE, by)[1]

    lane = lane_iota((ROWS, LANES))
    piece = LANES - lats
    extra = share - sent
    block = wide_ref.shape[0] * share // (2 * waves)

    def pack(m, _):
        def picked(i):
            return values_ref[pl.ds(m * (ROWS * share) + i, ROWS, stride=share), :]

        tails = [picked(sent + i) for i in range(extra)]
        for i in range(block):
            value = picked(i)
            if i < sent:
                value = jnp.where(lane < lats, value, pltpu.roll(tails[i % extra], lats - piece * (i // extra), 1))
            wide_ref[pl.ds(m * (ROWS * block) + i, ROWS, stride=block), :] = value
        return 0

    lax.fori_loop(0, wide_ref.shape[0] // (ROWS * block), pack, 0, unroll=PACK_UNROLL)
    out_ref[...] = wide_ref[...].astype(out_ref.dtype)


def unpack_kernel(in_ref, out_ref, zone_ref, flat_ref, *, lats, sent):
    share, levels, total = out_ref.shape
    bands = total // lats
    piece = LANES - lats
    extra = share - sent
    block = in_ref.shape[0] // (bands * levels)
    flat_ref[...] = in_ref[...].astype(jnp.float32)
    lane = lane_iota((levels, LANES))

    def rolled(value, shift):
        return value if shift % LANES == 0 else pltpu.roll(value, shift % LANES, 1)

    def picked(g, i):
        return flat_ref[pl.ds(g * levels * block + i, levels, stride=block), :]

    def pieces(c):
        for g in range(bands):
            if c < sent:
                yield picked(g, c), 0, g * lats, lats
            else:
                for j in range(sent // extra):
                    yield picked(g, j * extra + c - sent), lats, g * lats + piece * j, piece

    ends = [jnp.zeros((levels, LANES), jnp.float32) for _ in range(4)]
    for c in range(share):
        first = last = held = None
        for value, lo, lat, size in pieces(c):
            moved = rolled(value, lat - lo)
            fill = lat % LANES
            held = moved if fill == 0 else jnp.where(lane < fill, held, moved)
            if fill + size >= LANES:
                tile = lat // LANES
                out_ref[c, :, tile * LANES : (tile + 1) * LANES] = held
                first = held if tile == 0 else first
                last = held
                held = moved
        for e, (source, at) in enumerate(((last, LANES - 2), (last, LANES - 1), (first, 0), (first, 1))):
            ends[e] = jnp.where(lane == c, rolled(source, c - at), ends[e])
    for j in range(EXT_ZONE):
        step = jnp.full((levels, LANES), float(j + 1), jnp.float32) / (EXT_ZONE + 1.0)
        zone_ref[j] = blend(*ends, step)[:, :share]


def call(kernel, out_shape, scratch=(), limit=16 << 20, **static):
    return pl.pallas_call(
        functools.partial(kernel, **static),
        out_shape=out_shape,
        scratch_shapes=list(scratch),
        compiler_params=pltpu.CompilerParams(vmem_limit_bytes=limit),
        interpret=INTERPRET,
        name=kernel.__name__,
    )


def shards(level_field):
    blocks, bands = lax.axis_size("gx"), lax.axis_size("gy")
    levels, lats, cols = level_field.shape
    share = cols // bands
    coeffs = share * bands * blocks
    piece = LANES - lats
    parts = lats // piece
    sent = share * parts // (parts + 1)
    block = sent + sent % 2
    chunk = coeffs // 4
    bf16, f32 = jnp.bfloat16, jnp.float32
    assert share * bands == cols and levels == blocks == ROWS and lats == parts * piece
    assert sent * (parts + 1) == share * parts and cols == LANES + LANES // 2 and chunk % TILE == 0

    core = lax.all_to_all(level_field, "gx", split_axis=0, concat_axis=0, tiled=True)
    width = LANES * (blocks - 1)
    table = call(
        table_kernel,
        jax.ShapeDtypeStruct((coeffs + TILE, width), bf16),
        limit=8 << 20,
        blocks=blocks,
        cols=cols,
        chunk=chunk,
    )()
    dests = bands * blocks
    packed = call(
        transform_kernel,
        jax.ShapeDtypeStruct((dests * block, LANES), bf16),
        scratch=[
            pltpu.VMEM((2 * LANES, width), bf16),
            pltpu.VMEM((2, chunk, LANES), f32),
            pltpu.VMEM((coeffs + TILE, LANES), f32),
            pltpu.VMEM((dests * block, LANES), f32),
        ],
        chunk=chunk,
        share=share,
        sent=sent,
    )(core, table)
    packed = packed.reshape(dests, block // 2, 2, LANES)
    packed = lax.all_to_all(packed, ("gy", "gx"), split_axis=0, concat_axis=0, tiled=True)
    packed = packed.reshape(dests * block, LANES)
    spectra, zone = call(
        unpack_kernel,
        (
            jax.ShapeDtypeStruct((share, levels, lats * bands), f32),
            jax.ShapeDtypeStruct((EXT_ZONE, levels, share), f32),
        ),
        scratch=[pltpu.VMEM((dests * block, LANES), f32)],
        lats=lats,
        sent=sent,
    )(packed)
    return spectra, jnp.transpose(zone, (2, 1, 0))


def solution(mesh):
    coefficients = P(("gy", "gx"), ("member", "lev"), None)
    return jax.shard_map(
        shards,
        mesh=mesh,
        in_specs=(P(("member", "lev"), "gy", "gx"),),
        out_specs=(coefficients, coefficients),
        check_vma=False,
    )
```

```python
import functools
import math

import jax
import jax.numpy as jnp
from jax import lax
from jax.experimental import pallas as pl
from jax.experimental.pallas import tpu as pltpu
from jax.sharding import PartitionSpec as P

EXT_ZONE = 11
LANES = 128
ROWS = 8
TILE = 2 * ROWS
UNROLL = 4
PACK_UNROLL = 16
BAND_STEP = 13
INTERPRET = False


def blend(second_last, last_value, first_value, second_value, steps):
    weight_a = 2.0 * steps * steps * steps - 3.0 * steps * steps + 1.0
    weight_b = steps * steps * steps - 2.0 * steps * steps + steps
    weight_c = -2.0 * steps * steps * steps + 3.0 * steps * steps
    weight_d = steps * steps * steps - steps * steps
    scale = EXT_ZONE + 1.0
    slope_start = scale * (last_value - second_last)
    slope_end = scale * (second_value - first_value)
    return last_value * weight_a + slope_start * weight_b + first_value * weight_c + slope_end * weight_d


def sin_cos(turns, length):
    turns = turns - length * jnp.round(turns * (1.0 / length))
    half = turns * (math.pi / length)
    sq = half * half
    s = sq * (-1.0 / 39916800.0) + 1.0 / 362880.0
    s = s * sq - 1.0 / 5040.0
    s = s * sq + 1.0 / 120.0
    s = s * sq - 1.0 / 6.0
    s = (s * sq + 1.0) * half
    c = sq * (1.0 / 479001600.0) - 1.0 / 3628800.0
    c = c * sq + 1.0 / 40320.0
    c = c * sq - 1.0 / 720.0
    c = c * sq + 1.0 / 24.0
    c = c * sq - 0.5
    c = c * sq + 1.0
    return 2.0 * s * c, 1.0 - 2.0 * s * s


def lane_iota(shape):
    return lax.broadcasted_iota(jnp.int32, shape, 1)


def row_iota(shape):
    return lax.broadcasted_iota(jnp.int32, shape, 0)


def turned(at, by):
    c, s = at
    cb, sb = by
    return c * cb - s * sb, s * cb + c * sb


def twice(angle):
    c, s = angle
    return 1.0 - 2.0 * s * s, 2.0 * s * c


def table_kernel(table_ref, *, blocks, cols, chunk):
    length = blocks * cols + EXT_ZONE
    waves = blocks * cols // 2
    lane = lane_iota((TILE, LANES)).astype(jnp.float32)
    row = row_iota((TILE, LANES))
    scale = 1.0 / math.sqrt(length)

    def pairs(number):
        s, c = sin_cos(number * lane, float(length))
        mid = LANES // 2
        by_mid = jnp.broadcast_to(c[:, mid : mid + 1], c.shape), jnp.broadcast_to(s[:, mid : mid + 1], s.shape)
        by_lanes = twice(by_mid)
        by_block = turned(by_lanes, by_mid)
        near = (c * scale, s * scale)
        far = turned(near, by_lanes)
        side = turned(far, by_lanes)
        left = lane < float(mid)
        halves = blocks // 2
        yield halves * LANES, tuple(jnp.where(left, f, e) for f, e in zip(far, side))
        for b in range(halves):
            yield b * LANES, near
            if b >= 2:
                yield (halves + b - 1) * LANES, far
            near, far = turned(near, by_block), turned(far, by_block)

    per = chunk // TILE

    def rows(n, _):
        first = n // per * (2 * chunk) + n % per * TILE
        for lo, (c, s) in pairs((n * TILE + row).astype(jnp.float32)):
            for part, value in enumerate((c, -s)):
                at = pl.ds(pl.multiple_of(first + part * chunk, TILE), TILE)
                table_ref[at, lo : lo + LANES] = value.astype(table_ref.dtype)
        return 0

    lax.fori_loop(0, waves // TILE, rows, 0, unroll=UNROLL)
    for lo, (c, s) in pairs((waves + row % ROWS).astype(jnp.float32)):
        table_ref[2 * waves :, lo : lo + LANES] = jnp.where(row < ROWS, c, -s).astype(table_ref.dtype)


def transform_kernel(core_ref, table_ref, out_ref, rows_ref, turn_ref, values_ref, wide_ref, *, chunk, share, sent):
    blocks, lats, cols = core_ref.shape
    halves = blocks // 2
    length = blocks * cols + EXT_ZONE
    waves = blocks * cols // 2
    over = cols - LANES
    lane = lane_iota((lats, LANES))
    head = core_ref[0, :, :LANES].astype(jnp.float32)
    steps = (lane - over + 1).astype(jnp.float32) / (EXT_ZONE + 1.0)
    for part in range(2):
        lo = part * LANES
        rows_ref[lo + lats : lo + LANES, :] = jnp.zeros((LANES - lats, rows_ref.shape[1]), rows_ref.dtype)

        def place(tile, value):
            rows_ref[lo : lo + lats, tile * LANES : (tile + 1) * LANES] = value.astype(rows_ref.dtype)

        def others(b):
            value = core_ref[part * halves + b, :, LANES:].astype(jnp.float32)
            return jnp.concatenate([value, jnp.zeros((lats, LANES - over), jnp.float32)], axis=1)

        for b in range(halves):
            place(b, core_ref[part * halves + b, :, :LANES])
        place(halves, others(0) + pltpu.roll(others(1), over, 1))
        for b in range(2, halves):
            value = others(b)
            if part == 1 and b == halves - 1:
                zone = blend(value[:, over - 2 : over - 1], value[:, over - 1 : over], head[:, 0:1], head[:, 1:2], steps)
                value = jnp.where((lane >= over) & (lane < over + EXT_ZONE), zone, value)
            place(halves + b - 1, value)

    shift = float(halves * cols)
    s, c = sin_cos(row_iota((chunk, LANES)).astype(jnp.float32) * shift, float(length))
    turn_ref[0], turn_ref[1] = c, s
    step = 2.0 * math.pi * (chunk * halves * cols % length) / length
    step = math.cos(step), math.sin(step)

    def both(at, count, by):
        values = lax.dot_general(
            table_ref[at, :], rows_ref[...], (((1,), (1,)), ((), ())), preferred_element_type=jnp.float32
        )
        cb, sb = by
        c, s = values[: count // 2], values[count // 2 :]
        c_far, s_far = c[:, LANES:], s[:, LANES:]
        return c[:, :LANES] + (cb * c_far + sb * s_far), s[:, :LANES] + (cb * s_far - sb * c_far)

    def one(n, _):
        by = turn_ref[0], turn_ref[1]
        c, s = both(pl.ds(pl.multiple_of(n * (2 * chunk), 2 * chunk), 2 * chunk), 2 * chunk, by)
        values_ref[pl.ds(waves - 1 + n * chunk, chunk), :] = s
        values_ref[pl.ds(pl.multiple_of(n * chunk, chunk), chunk), :] = c
        turn_ref[0], turn_ref[1] = turned(by, step)
        return 0

    lax.fori_loop(0, waves // chunk, one, 0, unroll=2)
    by = turn_ref[0, :ROWS], turn_ref[1, :ROWS]
    values_ref[2 * waves - 1 : 2 * waves - 1 + ROWS, :] = both(slice(2 * waves, 2 * waves + TILE), TILE, by)[1]

    lane = lane_iota((ROWS, LANES))
    piece = LANES - lats
    extra = share - sent
    block = wide_ref.shape[0] * share // (2 * waves)
    bands = wide_ref.shape[0] // (ROWS * block)

    def pack(m, _):
        def picked(i):
            band = lax.rem(m * BAND_STEP, bands)
            return values_ref[pl.ds(band * (ROWS * share) + i, ROWS, stride=share), :]

        tails = [picked(sent + i) for i in range(extra)]
        for i in range(block):
            value = picked(i)
            if i < sent:
                value = jnp.where(lane < lats, value, pltpu.roll(tails[i % extra], lats - piece * (i // extra), 1))
            wide_ref[pl.ds(m * (ROWS * block) + i, ROWS, stride=block), :] = value
        return 0

    lax.fori_loop(0, bands, pack, 0, unroll=PACK_UNROLL)
    out_ref[...] = wide_ref[...].astype(out_ref.dtype)


def unpack_kernel(in_ref, out_hbm, zone_ref, flat_ref, out_ref, leaving, *, lats, sent):
    share, levels, total = out_ref.shape
    bands = total // lats
    piece = LANES - lats
    extra = share - sent
    block = in_ref.shape[0] // (bands * levels)
    flat_ref[...] = in_ref[...].astype(jnp.float32)
    lane = lane_iota((levels, LANES))

    def rolled(value, shift):
        return value if shift % LANES == 0 else pltpu.roll(value, shift % LANES, 1)

    def picked(g, i):
        return flat_ref[pl.ds(g * levels * block + i, levels, stride=block), :]

    def pieces(c):
        for g in range(bands):
            at = next(m for m in range(bands) if m * BAND_STEP % bands == g)
            if c < sent:
                yield picked(at, c), 0, g * lats, lats
            else:
                for j in range(sent // extra):
                    yield picked(at, j * extra + c - sent), lats, g * lats + piece * j, piece

    def send(c):
        return pltpu.make_async_copy(out_ref.at[c], out_hbm.at[c], leaving.at[c])

    ends = [jnp.zeros((levels, LANES), jnp.float32) for _ in range(4)]
    for c in range(share):
        first = last = held = None
        for value, lo, lat, size in pieces(c):
            moved = rolled(value, lat - lo)
            fill = lat % LANES
            held = moved if fill == 0 else jnp.where(lane < fill, held, moved)
            if fill + size >= LANES:
                tile = lat // LANES
                out_ref[c, :, tile * LANES : (tile + 1) * LANES] = held
                first = held if tile == 0 else first
                last = held
                held = moved
        send(c).start()
        for e, (source, at) in enumerate(((last, LANES - 2), (last, LANES - 1), (first, 0), (first, 1))):
            ends[e] = jnp.where(lane == c, rolled(source, c - at), ends[e])
    for j in range(EXT_ZONE):
        step = jnp.full((levels, LANES), float(j + 1), jnp.float32) / (EXT_ZONE + 1.0)
        zone_ref[j] = blend(*ends, step)[:, :share]
    for c in range(share):
        send(c).wait()


def call(kernel, out_shape, scratch=(), limit=16 << 20, **static):
    return pl.pallas_call(
        functools.partial(kernel, **static),
        out_shape=out_shape,
        scratch_shapes=list(scratch),
        compiler_params=pltpu.CompilerParams(vmem_limit_bytes=limit),
        interpret=INTERPRET,
        name=kernel.__name__,
    )


def shards(level_field):
    blocks, bands = lax.axis_size("gx"), lax.axis_size("gy")
    levels, lats, cols = level_field.shape
    share = cols // bands
    coeffs = share * bands * blocks
    piece = LANES - lats
    parts = lats // piece
    sent = share * parts // (parts + 1)
    block = sent + sent % 2
    chunk = coeffs // 4
    bf16, f32 = jnp.bfloat16, jnp.float32
    assert share * bands == cols and math.gcd(bands, BAND_STEP) == 1 and levels == blocks == ROWS and lats == parts * piece
    assert sent * (parts + 1) == share * parts and cols == LANES + LANES // 2 and chunk % TILE == 0

    core = lax.all_to_all(level_field, "gx", split_axis=0, concat_axis=0, tiled=True)
    width = LANES * (blocks - 1)
    table = call(
        table_kernel,
        jax.ShapeDtypeStruct((coeffs + TILE, width), bf16),
        limit=8 << 20,
        blocks=blocks,
        cols=cols,
        chunk=chunk,
    )()
    dests = bands * blocks
    packed = call(
        transform_kernel,
        jax.ShapeDtypeStruct((dests * block, LANES), bf16),
        scratch=[
            pltpu.VMEM((2 * LANES, width), bf16),
            pltpu.VMEM((2, chunk, LANES), f32),
            pltpu.VMEM((coeffs + TILE, LANES), f32),
            pltpu.VMEM((dests * block, LANES), f32),
        ],
        chunk=chunk,
        share=share,
        sent=sent,
    )(core, table)
    packed = packed.reshape(dests, block // 2, 2, LANES)
    order = [m * BAND_STEP % bands * blocks + x for m in range(bands) for x in range(blocks)]
    packed = lax.all_to_all(
        packed, ("gy", "gx"), split_axis=0, concat_axis=0, tiled=True, axis_index_groups=[order]
    )
    packed = packed.reshape(dests * block, LANES)
    spectra, zone = pl.pallas_call(
        functools.partial(unpack_kernel, lats=lats, sent=sent),
        out_shape=(
            jax.ShapeDtypeStruct((share, levels, lats * bands), f32),
            jax.ShapeDtypeStruct((EXT_ZONE, levels, share), f32),
        ),
        out_specs=(pl.BlockSpec(memory_space=pl.ANY), pl.BlockSpec(memory_space=pltpu.VMEM)),
        scratch_shapes=[
            pltpu.VMEM((dests * block, LANES), f32),
            pltpu.VMEM((share, levels, lats * bands), f32),
            pltpu.SemaphoreType.DMA((share,)),
        ],
        compiler_params=pltpu.CompilerParams(vmem_limit_bytes=16 << 20),
        interpret=INTERPRET,
        name="unpack_kernel",
    )(packed)
    return spectra, jnp.transpose(zone, (2, 1, 0))


def solution(mesh):
    coefficients = P(("gy", "gx"), ("member", "lev"), None)
    return jax.shard_map(
        shards,
        mesh=mesh,
        in_specs=(P(("member", "lev"), "gy", "gx"),),
        out_specs=(coefficients, coefficients),
        check_vma=False,
    )
```

```python
import functools
import math

import jax
import jax.numpy as jnp
from jax import lax
from jax.experimental import pallas as pl
from jax.experimental.pallas import tpu as pltpu
from jax.sharding import PartitionSpec as P

EXT_ZONE = 11
LANES = 128
ROWS = 8
TILE = 2 * ROWS
UNROLL = 4
PACK_UNROLL = 16
BAND_STEP = 13
INTERPRET = False


def blend(second_last, last_value, first_value, second_value, steps):
    weight_a = 2.0 * steps * steps * steps - 3.0 * steps * steps + 1.0
    weight_b = steps * steps * steps - 2.0 * steps * steps + steps
    weight_c = -2.0 * steps * steps * steps + 3.0 * steps * steps
    weight_d = steps * steps * steps - steps * steps
    scale = EXT_ZONE + 1.0
    slope_start = scale * (last_value - second_last)
    slope_end = scale * (second_value - first_value)
    return last_value * weight_a + slope_start * weight_b + first_value * weight_c + slope_end * weight_d


def sin_cos(turns, length):
    turns = turns - length * jnp.round(turns * (1.0 / length))
    half = turns * (math.pi / length)
    sq = half * half
    s = sq * (-1.0 / 39916800.0) + 1.0 / 362880.0
    s = s * sq - 1.0 / 5040.0
    s = s * sq + 1.0 / 120.0
    s = s * sq - 1.0 / 6.0
    s = (s * sq + 1.0) * half
    c = sq * (1.0 / 479001600.0) - 1.0 / 3628800.0
    c = c * sq + 1.0 / 40320.0
    c = c * sq - 1.0 / 720.0
    c = c * sq + 1.0 / 24.0
    c = c * sq - 0.5
    c = c * sq + 1.0
    return 2.0 * s * c, 1.0 - 2.0 * s * s


def lane_iota(shape):
    return lax.broadcasted_iota(jnp.int32, shape, 1)


def row_iota(shape):
    return lax.broadcasted_iota(jnp.int32, shape, 0)


def turned(at, by):
    c, s = at
    cb, sb = by
    return c * cb - s * sb, s * cb + c * sb


def twice(angle):
    c, s = angle
    return 1.0 - 2.0 * s * s, 2.0 * s * c


def table_kernel(table_ref, *, blocks, cols, chunk):
    length = blocks * cols + EXT_ZONE
    waves = blocks * cols // 2
    lane = lane_iota((TILE, LANES)).astype(jnp.float32)
    row = row_iota((TILE, LANES))
    scale = 1.0 / math.sqrt(length)

    def pairs(number):
        s, c = sin_cos(number * lane, float(length))
        mid = LANES // 2
        by_mid = jnp.broadcast_to(c[:, mid : mid + 1], c.shape), jnp.broadcast_to(s[:, mid : mid + 1], s.shape)
        by_lanes = twice(by_mid)
        by_block = turned(by_lanes, by_mid)
        near = (c * scale, s * scale)
        far = turned(near, by_lanes)
        side = turned(far, by_lanes)
        left = lane < float(mid)
        halves = blocks // 2
        yield halves * LANES, tuple(jnp.where(left, f, e) for f, e in zip(far, side))
        for b in range(halves):
            yield b * LANES, near
            if b >= 2:
                yield (halves + b - 1) * LANES, far
            near, far = turned(near, by_block), turned(far, by_block)

    per = chunk // TILE

    def rows(n, _):
        first = n // per * (2 * chunk) + n % per * TILE
        for lo, (c, s) in pairs((n * TILE + row).astype(jnp.float32)):
            for part, value in enumerate((c, -s)):
                at = pl.ds(pl.multiple_of(first + part * chunk, TILE), TILE)
                table_ref[at, lo : lo + LANES] = value.astype(table_ref.dtype)
        return 0

    lax.fori_loop(0, waves // TILE, rows, 0, unroll=UNROLL)
    for lo, (c, s) in pairs((waves + row % ROWS).astype(jnp.float32)):
        table_ref[2 * waves :, lo : lo + LANES] = jnp.where(row < ROWS, c, -s).astype(table_ref.dtype)


def transform_kernel(core_ref, table_ref, out_ref, rows_ref, turn_ref, values_ref, wide_ref, *, chunk, share, sent):
    blocks, lats, cols = core_ref.shape
    halves = blocks // 2
    length = blocks * cols + EXT_ZONE
    waves = blocks * cols // 2
    over = cols - LANES
    lane = lane_iota((lats, LANES))
    head = core_ref[0, :, :LANES].astype(jnp.float32)
    steps = (lane - over + 1).astype(jnp.float32) / (EXT_ZONE + 1.0)
    for part in range(2):
        lo = part * LANES
        rows_ref[lo + lats : lo + LANES, :] = jnp.zeros((LANES - lats, rows_ref.shape[1]), rows_ref.dtype)

        def place(tile, value):
            rows_ref[lo : lo + lats, tile * LANES : (tile + 1) * LANES] = value.astype(rows_ref.dtype)

        def others(b):
            value = core_ref[part * halves + b, :, LANES:].astype(jnp.float32)
            return jnp.concatenate([value, jnp.zeros((lats, LANES - over), jnp.float32)], axis=1)

        for b in range(halves):
            place(b, core_ref[part * halves + b, :, :LANES])
        place(halves, others(0) + pltpu.roll(others(1), over, 1))
        for b in range(2, halves):
            value = others(b)
            if part == 1 and b == halves - 1:
                zone = blend(value[:, over - 2 : over - 1], value[:, over - 1 : over], head[:, 0:1], head[:, 1:2], steps)
                value = jnp.where((lane >= over) & (lane < over + EXT_ZONE), zone, value)
            place(halves + b - 1, value)

    shift = float(halves * cols)
    s, c = sin_cos(row_iota((chunk, LANES)).astype(jnp.float32) * shift, float(length))
    turn_ref[0], turn_ref[1] = c, s
    step = 2.0 * math.pi * (chunk * halves * cols % length) / length
    step = math.cos(step), math.sin(step)

    def both(at, count, by):
        values = lax.dot_general(
            table_ref[at, :], rows_ref[...], (((1,), (1,)), ((), ())), preferred_element_type=jnp.float32
        )
        cb, sb = by
        c, s = values[: count // 2], values[count // 2 :]
        c_far, s_far = c[:, LANES:], s[:, LANES:]
        return c[:, :LANES] + (cb * c_far + sb * s_far), s[:, :LANES] + (cb * s_far - sb * c_far)

    def one(n, _):
        by = turn_ref[0], turn_ref[1]
        c, s = both(pl.ds(pl.multiple_of(n * (2 * chunk), 2 * chunk), 2 * chunk), 2 * chunk, by)
        values_ref[pl.ds(waves - 1 + n * chunk, chunk), :] = s
        values_ref[pl.ds(pl.multiple_of(n * chunk, chunk), chunk), :] = c
        turn_ref[0], turn_ref[1] = turned(by, step)
        return 0

    lax.fori_loop(0, waves // chunk, one, 0, unroll=2)
    by = turn_ref[0, :ROWS], turn_ref[1, :ROWS]
    values_ref[2 * waves - 1 : 2 * waves - 1 + ROWS, :] = both(slice(2 * waves, 2 * waves + TILE), TILE, by)[1]

    lane = lane_iota((ROWS, LANES))
    piece = LANES - lats
    extra = share - sent
    block = wide_ref.shape[0] * share // (2 * waves)
    bands = wide_ref.shape[0] // (ROWS * block)

    def pack(m, _):
        def picked(i):
            band = lax.rem(m * BAND_STEP, bands)
            return values_ref[pl.ds(band * (ROWS * share) + i, ROWS, stride=share), :]

        tails = [picked(sent + i) for i in range(extra)]
        for i in range(block):
            value = picked(i)
            if i < sent:
                value = jnp.where(lane < lats, value, pltpu.roll(tails[i % extra], lats - piece * (i // extra), 1))
            wide_ref[pl.ds(m * (ROWS * block) + i, ROWS, stride=block), :] = value
        return 0

    lax.fori_loop(0, bands, pack, 0, unroll=PACK_UNROLL)
    out_ref[...] = wide_ref[...].astype(out_ref.dtype)


def unpack_kernel(in_ref, out_ref, zone_ref, flat_ref, *, lats, sent):
    share, levels, total = out_ref.shape
    bands = total // lats
    piece = LANES - lats
    extra = share - sent
    block = in_ref.shape[0] // (bands * levels)
    flat_ref[...] = in_ref[...].astype(jnp.float32)
    lane = lane_iota((levels, LANES))

    def rolled(value, shift):
        return value if shift % LANES == 0 else pltpu.roll(value, shift % LANES, 1)

    def picked(g, i):
        return flat_ref[pl.ds(g * levels * block + i, levels, stride=block), :]

    def pieces(c):
        for g in range(bands):
            at = next(m for m in range(bands) if m * BAND_STEP % bands == g)
            if c < sent:
                yield picked(at, c), 0, g * lats, lats
            else:
                for j in range(sent // extra):
                    yield picked(at, j * extra + c - sent), lats, g * lats + piece * j, piece

    ends = [jnp.zeros((levels, LANES), jnp.float32) for _ in range(4)]
    for c in range(share):
        first = last = held = None
        for value, lo, lat, size in pieces(c):
            moved = rolled(value, lat - lo)
            fill = lat % LANES
            held = moved if fill == 0 else jnp.where(lane < fill, held, moved)
            if fill + size >= LANES:
                tile = lat // LANES
                out_ref[c, :, tile * LANES : (tile + 1) * LANES] = held
                first = held if tile == 0 else first
                last = held
                held = moved
        for e, (source, at) in enumerate(((last, LANES - 2), (last, LANES - 1), (first, 0), (first, 1))):
            ends[e] = jnp.where(lane == c, rolled(source, c - at), ends[e])
    for j in range(EXT_ZONE):
        step = jnp.full((levels, LANES), float(j + 1), jnp.float32) / (EXT_ZONE + 1.0)
        zone_ref[j] = blend(*ends, step)[:, :share]


def call(kernel, out_shape, scratch=(), limit=16 << 20, **static):
    return pl.pallas_call(
        functools.partial(kernel, **static),
        out_shape=out_shape,
        scratch_shapes=list(scratch),
        compiler_params=pltpu.CompilerParams(vmem_limit_bytes=limit),
        interpret=INTERPRET,
        name=kernel.__name__,
    )


def shards(level_field):
    blocks, bands = lax.axis_size("gx"), lax.axis_size("gy")
    levels, lats, cols = level_field.shape
    share = cols // bands
    coeffs = share * bands * blocks
    piece = LANES - lats
    parts = lats // piece
    sent = share * parts // (parts + 1)
    block = sent + sent % 2
    chunk = coeffs // 4
    bf16, f32 = jnp.bfloat16, jnp.float32
    assert share * bands == cols and math.gcd(bands, BAND_STEP) == 1 and levels == blocks == ROWS and lats == parts * piece
    assert sent * (parts + 1) == share * parts and cols == LANES + LANES // 2 and chunk % TILE == 0

    core = lax.all_to_all(level_field, "gx", split_axis=0, concat_axis=0, tiled=True)
    width = LANES * (blocks - 1)
    table = call(
        table_kernel,
        jax.ShapeDtypeStruct((coeffs + TILE, width), bf16),
        limit=8 << 20,
        blocks=blocks,
        cols=cols,
        chunk=chunk,
    )()
    dests = bands * blocks
    packed = call(
        transform_kernel,
        jax.ShapeDtypeStruct((dests * block, LANES), bf16),
        scratch=[
            pltpu.VMEM((2 * LANES, width), bf16),
            pltpu.VMEM((2, chunk, LANES), f32),
            pltpu.VMEM((coeffs + TILE, LANES), f32),
            pltpu.VMEM((dests * block, LANES), f32),
        ],
        chunk=chunk,
        share=share,
        sent=sent,
    )(core, table)
    packed = packed.reshape(dests, block // 2, 2, LANES)
    order = [m * BAND_STEP % bands * blocks + x for m in range(bands) for x in range(blocks)]
    packed = lax.all_to_all(
        packed, ("gy", "gx"), split_axis=0, concat_axis=0, tiled=True, axis_index_groups=[order]
    )
    packed = packed.reshape(dests * block, LANES)
    spectra, zone = call(
        unpack_kernel,
        (
            jax.ShapeDtypeStruct((share, levels, lats * bands), f32),
            jax.ShapeDtypeStruct((EXT_ZONE, levels, share), f32),
        ),
        scratch=[pltpu.VMEM((dests * block, LANES), f32)],
        lats=lats,
        sent=sent,
    )(packed)
    return spectra, jnp.transpose(zone, (2, 1, 0))


def solution(mesh):
    coefficients = P(("gy", "gx"), ("member", "lev"), None)
    return jax.shard_map(
        shards,
        mesh=mesh,
        in_specs=(P(("member", "lev"), "gy", "gx"),),
        out_specs=(coefficients, coefficients),
        check_vma=False,
    )
```

```python
import functools
import math

import jax
import jax.numpy as jnp
from jax import lax
from jax.experimental import pallas as pl
from jax.experimental.pallas import tpu as pltpu
from jax.sharding import PartitionSpec as P

EXT_ZONE = 11
LANES = 128
ROWS = 8
TILE = 2 * ROWS
UNROLL = 4
PACK_UNROLL = 16
BAND_STEP = 13
INTERPRET = False


def blend(second_last, last_value, first_value, second_value, steps):
    weight_a = 2.0 * steps * steps * steps - 3.0 * steps * steps + 1.0
    weight_b = steps * steps * steps - 2.0 * steps * steps + steps
    weight_c = -2.0 * steps * steps * steps + 3.0 * steps * steps
    weight_d = steps * steps * steps - steps * steps
    scale = EXT_ZONE + 1.0
    slope_start = scale * (last_value - second_last)
    slope_end = scale * (second_value - first_value)
    return last_value * weight_a + slope_start * weight_b + first_value * weight_c + slope_end * weight_d


def sin_cos(turns, length):
    turns = turns - length * jnp.round(turns * (1.0 / length))
    half = turns * (math.pi / length)
    sq = half * half
    s = sq * (-1.0 / 39916800.0) + 1.0 / 362880.0
    s = s * sq - 1.0 / 5040.0
    s = s * sq + 1.0 / 120.0
    s = s * sq - 1.0 / 6.0
    s = (s * sq + 1.0) * half
    c = sq * (1.0 / 479001600.0) - 1.0 / 3628800.0
    c = c * sq + 1.0 / 40320.0
    c = c * sq - 1.0 / 720.0
    c = c * sq + 1.0 / 24.0
    c = c * sq - 0.5
    c = c * sq + 1.0
    return 2.0 * s * c, 1.0 - 2.0 * s * s


def lane_iota(shape):
    return lax.broadcasted_iota(jnp.int32, shape, 1)


def row_iota(shape):
    return lax.broadcasted_iota(jnp.int32, shape, 0)


def turned(at, by):
    c, s = at
    cb, sb = by
    return c * cb - s * sb, s * cb + c * sb


def twice(angle):
    c, s = angle
    return 1.0 - 2.0 * s * s, 2.0 * s * c


def table_kernel(table_ref, *, blocks, cols, chunk):
    length = blocks * cols + EXT_ZONE
    waves = blocks * cols // 2
    lane = lane_iota((TILE, LANES)).astype(jnp.float32)
    row = row_iota((TILE, LANES))
    scale = 1.0 / math.sqrt(length)

    def pairs(number):
        s, c = sin_cos(number * lane, float(length))
        mid = LANES // 2
        by_mid = jnp.broadcast_to(c[:, mid : mid + 1], c.shape), jnp.broadcast_to(s[:, mid : mid + 1], s.shape)
        by_lanes = twice(by_mid)
        by_block = turned(by_lanes, by_mid)
        near = (c * scale, s * scale)
        far = turned(near, by_lanes)
        side = turned(far, by_lanes)
        left = lane < float(mid)
        halves = blocks // 2
        yield halves * LANES, tuple(jnp.where(left, f, e) for f, e in zip(far, side))
        for b in range(halves):
            yield b * LANES, near
            if b >= 2:
                yield (halves + b - 1) * LANES, far
            near, far = turned(near, by_block), turned(far, by_block)

    per = chunk // TILE

    def rows(n, _):
        first = n // per * (2 * chunk) + n % per * TILE
        for lo, (c, s) in pairs((n * TILE + row).astype(jnp.float32)):
            for part, value in enumerate((c, -s)):
                at = pl.ds(pl.multiple_of(first + part * chunk, TILE), TILE)
                table_ref[at, lo : lo + LANES] = value.astype(table_ref.dtype)
        return 0

    lax.fori_loop(0, waves // TILE, rows, 0, unroll=UNROLL)
    for lo, (c, s) in pairs((waves + row % ROWS).astype(jnp.float32)):
        table_ref[2 * waves :, lo : lo + LANES] = jnp.where(row < ROWS, c, -s).astype(table_ref.dtype)


def transform_kernel(core_ref, table_ref, out_ref, rows_ref, turn_ref, values_ref, wide_ref, *, chunk, share, sent):
    blocks, lats, cols = core_ref.shape
    halves = blocks // 2
    length = blocks * cols + EXT_ZONE
    waves = blocks * cols // 2
    over = cols - LANES
    lane = lane_iota((lats, LANES))
    head = core_ref[0, :, :LANES].astype(jnp.float32)
    steps = (lane - over + 1).astype(jnp.float32) / (EXT_ZONE + 1.0)
    for part in range(2):
        lo = part * LANES
        rows_ref[lo + lats : lo + LANES, :] = jnp.zeros((LANES - lats, rows_ref.shape[1]), rows_ref.dtype)

        def place(tile, value):
            rows_ref[lo : lo + lats, tile * LANES : (tile + 1) * LANES] = value.astype(rows_ref.dtype)

        def others(b):
            value = core_ref[part * halves + b, :, LANES:].astype(jnp.float32)
            return jnp.concatenate([value, jnp.zeros((lats, LANES - over), jnp.float32)], axis=1)

        for b in range(halves):
            place(b, core_ref[part * halves + b, :, :LANES])
        place(halves, others(0) + pltpu.roll(others(1), over, 1))
        for b in range(2, halves):
            value = others(b)
            if part == 1 and b == halves - 1:
                zone = blend(value[:, over - 2 : over - 1], value[:, over - 1 : over], head[:, 0:1], head[:, 1:2], steps)
                value = jnp.where((lane >= over) & (lane < over + EXT_ZONE), zone, value)
            place(halves + b - 1, value)

    shift = float(halves * cols)
    s, c = sin_cos(row_iota((chunk, LANES)).astype(jnp.float32) * shift, float(length))
    turn_ref[0], turn_ref[1] = c, s
    step = 2.0 * math.pi * (chunk * halves * cols % length) / length
    step = math.cos(step), math.sin(step)

    def both(at, count, by):
        values = lax.dot_general(
            table_ref[at, :], rows_ref[...], (((1,), (1,)), ((), ())), preferred_element_type=jnp.float32
        )
        cb, sb = by
        c, s = values[: count // 2], values[count // 2 :]
        c_far, s_far = c[:, LANES:], s[:, LANES:]
        return c[:, :LANES] + (cb * c_far + sb * s_far), s[:, :LANES] + (cb * s_far - sb * c_far)

    def one(n, _):
        by = turn_ref[0], turn_ref[1]
        c, s = both(pl.ds(pl.multiple_of(n * (2 * chunk), 2 * chunk), 2 * chunk), 2 * chunk, by)
        values_ref[pl.ds(waves - 1 + n * chunk, chunk), :] = s
        values_ref[pl.ds(pl.multiple_of(n * chunk, chunk), chunk), :] = c
        turn_ref[0], turn_ref[1] = turned(by, step)
        return 0

    lax.fori_loop(0, waves // chunk, one, 0, unroll=2)
    by = turn_ref[0, :ROWS], turn_ref[1, :ROWS]
    values_ref[2 * waves - 1 : 2 * waves - 1 + ROWS, :] = both(slice(2 * waves, 2 * waves + TILE), TILE, by)[1]

    lane = lane_iota((ROWS, LANES))
    piece = LANES - lats
    extra = share - sent
    block = wide_ref.shape[0] * share // (2 * waves)
    bands = wide_ref.shape[0] // (ROWS * block)

    def pack(m, _):
        def picked(i):
            band = lax.rem(m * BAND_STEP, bands)
            return values_ref[pl.ds(band * (ROWS * share) + i, ROWS, stride=share), :]

        tails = [picked(sent + i) for i in range(extra)]
        for i in range(block):
            value = picked(i)
            if i < sent:
                value = jnp.where(lane < lats, value, pltpu.roll(tails[i % extra], lats - piece * (i // extra), 1))
            wide_ref[pl.ds(m * (ROWS * block) + i, ROWS, stride=block), :] = value
        return 0

    lax.fori_loop(0, bands, pack, 0, unroll=PACK_UNROLL)
    out_ref[...] = wide_ref[...].astype(out_ref.dtype)


def unpack_kernel(in_ref, out_ref, zone_ref, flat_ref, *, lats, sent):
    share, levels, total = out_ref.shape
    bands = total // lats
    piece = LANES - lats
    extra = share - sent
    block = in_ref.shape[0] // (bands * levels)
    flat_ref[...] = in_ref[...].astype(jnp.float32)
    lane = lane_iota((levels, LANES))

    def rolled(value, shift):
        return value if shift % LANES == 0 else pltpu.roll(value, shift % LANES, 1)

    def picked(g, i):
        return flat_ref[pl.ds(g * levels * block + i, levels, stride=block), :]

    ends = [jnp.zeros((levels, LANES), jnp.float32) for _ in range(4)]
    held = [None] * share

    def place(c, value, lo, lat, size):
        moved = rolled(value, lat - lo)
        fill = lat % LANES
        held[c] = moved if fill == 0 else jnp.where(lane < fill, held[c], moved)
        if fill + size >= LANES:
            tile = lat // LANES
            out_ref[c, :, tile * LANES : (tile + 1) * LANES] = held[c]
            for e, (edge, at) in enumerate(((total // LANES - 1, LANES - 2), (total // LANES - 1, LANES - 1), (0, 0), (0, 1))):
                if tile == edge:
                    ends[e] = jnp.where(lane == c, rolled(held[c], c - at), ends[e])
            held[c] = moved

    for i in range(extra):
        for g in range(bands):
            at = next(m for m in range(bands) if m * BAND_STEP % bands == g)
            for j in range(sent // extra):
                value = picked(at, j * extra + i)
                place(j * extra + i, value, 0, g * lats, lats)
                place(sent + i, value, lats, g * lats + piece * j, piece)
    for j in range(EXT_ZONE):
        step = jnp.full((levels, LANES), float(j + 1), jnp.float32) / (EXT_ZONE + 1.0)
        zone_ref[j] = blend(*ends, step)[:, :share]


def call(kernel, out_shape, scratch=(), limit=16 << 20, **static):
    return pl.pallas_call(
        functools.partial(kernel, **static),
        out_shape=out_shape,
        scratch_shapes=list(scratch),
        compiler_params=pltpu.CompilerParams(vmem_limit_bytes=limit),
        interpret=INTERPRET,
        name=kernel.__name__,
    )


def shards(level_field):
    blocks, bands = lax.axis_size("gx"), lax.axis_size("gy")
    levels, lats, cols = level_field.shape
    share = cols // bands
    coeffs = share * bands * blocks
    piece = LANES - lats
    parts = lats // piece
    sent = share * parts // (parts + 1)
    block = sent + sent % 2
    chunk = coeffs // 4
    bf16, f32 = jnp.bfloat16, jnp.float32
    assert share * bands == cols and math.gcd(bands, BAND_STEP) == 1 and levels == blocks == ROWS and lats == parts * piece
    assert sent * (parts + 1) == share * parts and cols == LANES + LANES // 2 and chunk % TILE == 0

    core = lax.all_to_all(level_field, "gx", split_axis=0, concat_axis=0, tiled=True)
    width = LANES * (blocks - 1)
    table = call(
        table_kernel,
        jax.ShapeDtypeStruct((coeffs + TILE, width), bf16),
        limit=8 << 20,
        blocks=blocks,
        cols=cols,
        chunk=chunk,
    )()
    dests = bands * blocks
    packed = call(
        transform_kernel,
        jax.ShapeDtypeStruct((dests * block, LANES), bf16),
        scratch=[
            pltpu.VMEM((2 * LANES, width), bf16),
            pltpu.VMEM((2, chunk, LANES), f32),
            pltpu.VMEM((coeffs + TILE, LANES), f32),
            pltpu.VMEM((dests * block, LANES), f32),
        ],
        chunk=chunk,
        share=share,
        sent=sent,
    )(core, table)
    packed = packed.reshape(dests, block // 2, 2, LANES)
    order = [m * BAND_STEP % bands * blocks + x for m in range(bands) for x in range(blocks)]
    packed = lax.all_to_all(
        packed, ("gy", "gx"), split_axis=0, concat_axis=0, tiled=True, axis_index_groups=[order]
    )
    packed = packed.reshape(dests * block, LANES)
    spectra, zone = call(
        unpack_kernel,
        (
            jax.ShapeDtypeStruct((share, levels, lats * bands), f32),
            jax.ShapeDtypeStruct((EXT_ZONE, levels, share), f32),
        ),
        scratch=[pltpu.VMEM((dests * block, LANES), f32)],
        lats=lats,
        sent=sent,
    )(packed)
    return spectra, jnp.transpose(zone, (2, 1, 0))


def solution(mesh):
    coefficients = P(("gy", "gx"), ("member", "lev"), None)
    return jax.shard_map(
        shards,
        mesh=mesh,
        in_specs=(P(("member", "lev"), "gy", "gx"),),
        out_specs=(coefficients, coefficients),
        check_vma=False,
    )
```

```python
import functools
import math

import jax
import jax.numpy as jnp
from jax import lax
from jax.experimental import pallas as pl
from jax.experimental.pallas import tpu as pltpu
from jax.sharding import PartitionSpec as P

EXT_ZONE = 11
LANES = 128
ROWS = 8
TILE = 2 * ROWS
UNROLL = 4
PACK_UNROLL = 16
BAND_STEP = 3
INTERPRET = False


def blend(second_last, last_value, first_value, second_value, steps):
    weight_a = 2.0 * steps * steps * steps - 3.0 * steps * steps + 1.0
    weight_b = steps * steps * steps - 2.0 * steps * steps + steps
    weight_c = -2.0 * steps * steps * steps + 3.0 * steps * steps
    weight_d = steps * steps * steps - steps * steps
    scale = EXT_ZONE + 1.0
    slope_start = scale * (last_value - second_last)
    slope_end = scale * (second_value - first_value)
    return last_value * weight_a + slope_start * weight_b + first_value * weight_c + slope_end * weight_d


def sin_cos(turns, length):
    turns = turns - length * jnp.round(turns * (1.0 / length))
    half = turns * (math.pi / length)
    sq = half * half
    s = sq * (-1.0 / 39916800.0) + 1.0 / 362880.0
    s = s * sq - 1.0 / 5040.0
    s = s * sq + 1.0 / 120.0
    s = s * sq - 1.0 / 6.0
    s = (s * sq + 1.0) * half
    c = sq * (1.0 / 479001600.0) - 1.0 / 3628800.0
    c = c * sq + 1.0 / 40320.0
    c = c * sq - 1.0 / 720.0
    c = c * sq + 1.0 / 24.0
    c = c * sq - 0.5
    c = c * sq + 1.0
    return 2.0 * s * c, 1.0 - 2.0 * s * s


def lane_iota(shape):
    return lax.broadcasted_iota(jnp.int32, shape, 1)


def row_iota(shape):
    return lax.broadcasted_iota(jnp.int32, shape, 0)


def turned(at, by):
    c, s = at
    cb, sb = by
    return c * cb - s * sb, s * cb + c * sb


def twice(angle):
    c, s = angle
    return 1.0 - 2.0 * s * s, 2.0 * s * c


def table_kernel(table_ref, *, blocks, cols, chunk):
    length = blocks * cols + EXT_ZONE
    waves = blocks * cols // 2
    lane = lane_iota((TILE, LANES)).astype(jnp.float32)
    row = row_iota((TILE, LANES))
    scale = 1.0 / math.sqrt(length)

    def pairs(number):
        s, c = sin_cos(number * lane, float(length))
        mid = LANES // 2
        by_mid = jnp.broadcast_to(c[:, mid : mid + 1], c.shape), jnp.broadcast_to(s[:, mid : mid + 1], s.shape)
        by_lanes = twice(by_mid)
        by_block = turned(by_lanes, by_mid)
        near = (c * scale, s * scale)
        far = turned(near, by_lanes)
        side = turned(far, by_lanes)
        left = lane < float(mid)
        halves = blocks // 2
        yield halves * LANES, tuple(jnp.where(left, f, e) for f, e in zip(far, side))
        for b in range(halves):
            yield b * LANES, near
            if b >= 2:
                yield (halves + b - 1) * LANES, far
            near, far = turned(near, by_block), turned(far, by_block)

    per = chunk // TILE

    def rows(n, _):
        first = n // per * (2 * chunk) + n % per * TILE
        for lo, (c, s) in pairs((n * TILE + row).astype(jnp.float32)):
            for part, value in enumerate((c, -s)):
                at = pl.ds(pl.multiple_of(first + part * chunk, TILE), TILE)
                table_ref[at, lo : lo + LANES] = value.astype(table_ref.dtype)
        return 0

    lax.fori_loop(0, waves // TILE, rows, 0, unroll=UNROLL)
    for lo, (c, s) in pairs((waves + row % ROWS).astype(jnp.float32)):
        table_ref[2 * waves :, lo : lo + LANES] = jnp.where(row < ROWS, c, -s).astype(table_ref.dtype)


def transform_kernel(core_ref, table_ref, out_ref, rows_ref, turn_ref, values_ref, wide_ref, *, chunk, share, sent):
    blocks, lats, cols = core_ref.shape
    halves = blocks // 2
    length = blocks * cols + EXT_ZONE
    waves = blocks * cols // 2
    over = cols - LANES
    lane = lane_iota((lats, LANES))
    head = core_ref[0, :, :LANES].astype(jnp.float32)
    steps = (lane - over + 1).astype(jnp.float32) / (EXT_ZONE + 1.0)
    for part in range(2):
        lo = part * LANES
        rows_ref[lo + lats : lo + LANES, :] = jnp.zeros((LANES - lats, rows_ref.shape[1]), rows_ref.dtype)

        def place(tile, value):
            rows_ref[lo : lo + lats, tile * LANES : (tile + 1) * LANES] = value.astype(rows_ref.dtype)

        def others(b):
            value = core_ref[part * halves + b, :, LANES:].astype(jnp.float32)
            return jnp.concatenate([value, jnp.zeros((lats, LANES - over), jnp.float32)], axis=1)

        for b in range(halves):
            place(b, core_ref[part * halves + b, :, :LANES])
        place(halves, others(0) + pltpu.roll(others(1), over, 1))
        for b in range(2, halves):
            value = others(b)
            if part == 1 and b == halves - 1:
                zone = blend(value[:, over - 2 : over - 1], value[:, over - 1 : over], head[:, 0:1], head[:, 1:2], steps)
                value = jnp.where((lane >= over) & (lane < over + EXT_ZONE), zone, value)
            place(halves + b - 1, value)

    shift = float(halves * cols)
    s, c = sin_cos(row_iota((chunk, LANES)).astype(jnp.float32) * shift, float(length))
    turn_ref[0], turn_ref[1] = c, s
    step = 2.0 * math.pi * (chunk * halves * cols % length) / length
    step = math.cos(step), math.sin(step)

    def both(at, count, by):
        values = lax.dot_general(
            table_ref[at, :], rows_ref[...], (((1,), (1,)), ((), ())), preferred_element_type=jnp.float32
        )
        cb, sb = by
        c, s = values[: count // 2], values[count // 2 :]
        c_far, s_far = c[:, LANES:], s[:, LANES:]
        return c[:, :LANES] + (cb * c_far + sb * s_far), s[:, :LANES] + (cb * s_far - sb * c_far)

    def one(n, _):
        by = turn_ref[0], turn_ref[1]
        c, s = both(pl.ds(pl.multiple_of(n * (2 * chunk), 2 * chunk), 2 * chunk), 2 * chunk, by)
        values_ref[pl.ds(waves - 1 + n * chunk, chunk), :] = s
        values_ref[pl.ds(pl.multiple_of(n * chunk, chunk), chunk), :] = c
        turn_ref[0], turn_ref[1] = turned(by, step)
        return 0

    lax.fori_loop(0, waves // chunk, one, 0, unroll=2)
    by = turn_ref[0, :ROWS], turn_ref[1, :ROWS]
    values_ref[2 * waves - 1 : 2 * waves - 1 + ROWS, :] = both(slice(2 * waves, 2 * waves + TILE), TILE, by)[1]

    lane = lane_iota((ROWS, LANES))
    piece = LANES - lats
    extra = share - sent
    block = wide_ref.shape[0] * share // (2 * waves)
    bands = wide_ref.shape[0] // (ROWS * block)

    def pack(m, _):
        def picked(i):
            band = lax.rem(m * BAND_STEP, bands)
            return values_ref[pl.ds(band * (ROWS * share) + i, ROWS, stride=share), :]

        tails = [picked(sent + i) for i in range(extra)]
        for i in range(block):
            value = picked(i)
            if i < sent:
                value = jnp.where(lane < lats, value, pltpu.roll(tails[i % extra], lats - piece * (i // extra), 1))
            wide_ref[pl.ds(m * (ROWS * block) + i, ROWS, stride=block), :] = value
        return 0

    lax.fori_loop(0, bands, pack, 0, unroll=PACK_UNROLL)
    out_ref[...] = wide_ref[...].astype(out_ref.dtype)


def unpack_kernel(in_ref, out_ref, zone_ref, flat_ref, *, lats, sent):
    share, levels, total = out_ref.shape
    bands = total // lats
    piece = LANES - lats
    extra = share - sent
    block = in_ref.shape[0] // (bands * levels)
    flat_ref[...] = in_ref[...].astype(jnp.float32)
    lane = lane_iota((levels, LANES))

    def rolled(value, shift):
        return value if shift % LANES == 0 else pltpu.roll(value, shift % LANES, 1)

    def picked(g, i):
        return flat_ref[pl.ds(g * levels * block + i, levels, stride=block), :]

    def pieces(c):
        for g in range(bands):
            at = next(m for m in range(bands) if m * BAND_STEP % bands == g)
            if c < sent:
                yield picked(at, c), 0, g * lats, lats
            else:
                for j in range(sent // extra):
                    yield picked(at, j * extra + c - sent), lats, g * lats + piece * j, piece

    ends = [jnp.zeros((levels, LANES), jnp.float32) for _ in range(4)]
    for c in range(share):
        first = last = held = None
        for value, lo, lat, size in pieces(c):
            moved = rolled(value, lat - lo)
            fill = lat % LANES
            held = moved if fill == 0 else jnp.where(lane < fill, held, moved)
            if fill + size >= LANES:
                tile = lat // LANES
                out_ref[c, :, tile * LANES : (tile + 1) * LANES] = held
                first = held if tile == 0 else first
                last = held
                held = moved
        for e, (source, at) in enumerate(((last, LANES - 2), (last, LANES - 1), (first, 0), (first, 1))):
            ends[e] = jnp.where(lane == c, rolled(source, c - at), ends[e])
    for j in range(EXT_ZONE):
        step = jnp.full((levels, LANES), float(j + 1), jnp.float32) / (EXT_ZONE + 1.0)
        zone_ref[j] = blend(*ends, step)[:, :share]


def call(kernel, out_shape, scratch=(), limit=16 << 20, **static):
    return pl.pallas_call(
        functools.partial(kernel, **static),
        out_shape=out_shape,
        scratch_shapes=list(scratch),
        compiler_params=pltpu.CompilerParams(vmem_limit_bytes=limit),
        interpret=INTERPRET,
        name=kernel.__name__,
    )


def shards(level_field):
    blocks, bands = lax.axis_size("gx"), lax.axis_size("gy")
    levels, lats, cols = level_field.shape
    share = cols // bands
    coeffs = share * bands * blocks
    piece = LANES - lats
    parts = lats // piece
    sent = share * parts // (parts + 1)
    block = sent + sent % 2
    chunk = coeffs // 4
    bf16, f32 = jnp.bfloat16, jnp.float32
    assert share * bands == cols and math.gcd(bands, BAND_STEP) == 1 and levels == blocks == ROWS and lats == parts * piece
    assert sent * (parts + 1) == share * parts and cols == LANES + LANES // 2 and chunk % TILE == 0

    core = lax.all_to_all(level_field, "gx", split_axis=0, concat_axis=0, tiled=True)
    width = LANES * (blocks - 1)
    table = call(
        table_kernel,
        jax.ShapeDtypeStruct((coeffs + TILE, width), bf16),
        limit=8 << 20,
        blocks=blocks,
        cols=cols,
        chunk=chunk,
    )()
    dests = bands * blocks
    packed = call(
        transform_kernel,
        jax.ShapeDtypeStruct((dests * block, LANES), bf16),
        scratch=[
            pltpu.VMEM((2 * LANES, width), bf16),
            pltpu.VMEM((2, chunk, LANES), f32),
            pltpu.VMEM((coeffs + TILE, LANES), f32),
            pltpu.VMEM((dests * block, LANES), f32),
        ],
        chunk=chunk,
        share=share,
        sent=sent,
    )(core, table)
    packed = packed.reshape(dests, block // 2, 2, LANES)
    order = [m * BAND_STEP % bands * blocks + x for m in range(bands) for x in range(blocks)]
    packed = lax.all_to_all(
        packed, ("gy", "gx"), split_axis=0, concat_axis=0, tiled=True, axis_index_groups=[order]
    )
    packed = packed.reshape(dests * block, LANES)
    spectra, zone = call(
        unpack_kernel,
        (
            jax.ShapeDtypeStruct((share, levels, lats * bands), f32),
            jax.ShapeDtypeStruct((EXT_ZONE, levels, share), f32),
        ),
        scratch=[pltpu.VMEM((dests * block, LANES), f32)],
        lats=lats,
        sent=sent,
    )(packed)
    return spectra, jnp.transpose(zone, (2, 1, 0))


def solution(mesh):
    coefficients = P(("gy", "gx"), ("member", "lev"), None)
    return jax.shard_map(
        shards,
        mesh=mesh,
        in_specs=(P(("member", "lev"), "gy", "gx"),),
        out_specs=(coefficients, coefficients),
        check_vma=False,
    )
```
